256 devices in a mesh: groups: 4 (over x, y), ep: 64 (over z, core).
Axes of the slice: x: 2, y: 2, z: 32, core: 2. Of those that a mesh axis runs over, the one named last changes fastest.
The devices are a block of a 4x8x32 slice.
Arguments:
- tokens: bfloat16 [16384, 2880], P(('groups', 'ep')), parts along dimension 0, may hold values from -6 to 6
- routes: int32 [16384, 4], P(('groups', 'ep')), parts along dimension 0, may hold values from 0 to 15, all different within a row; in each aligned block of 64 rows (0 to 63, 64 to 127, ...) at most 20 rows name the same one
- norm_gain: bfloat16 [2880], replicated, may hold values from 0.25 to 1.75
- router_weight: bfloat16 [2880, 16], replicated, may hold values from -0.02734375 to 0.02734375
- gate_up_weight: bfloat16 [64, 2880, 720], P('ep'), may hold values from -0.109375 to 0.109375
- down_weight: bfloat16 [64, 360, 2880], P('ep'), may hold values from -0.15625 to 0.15625
Outputs:
- mixed: bfloat16 [16384, 2880], P(('groups', 'ep')), parts along dimension 0
The draws below stay inside these ranges and needn't reach their ends.
There are 4 independent parts, one for each index of `groups`. The reference program is written for one: setup_inputs(seed, part) draws one part's arguments, and reference() takes and returns one part's arrays. A program takes and returns all parts, laid end to end along the dimension named above; an argument that names none is the same for every part. Nothing has to cross between parts.
Inputs may be any that keep to these rules, and one draw needn't show every extreme that they name: `routes`: in each aligned block of 64 rows (the rows of one device), no expert is named by more than 20 rows; in some blocks one expert is named by exactly 20 rows. A row names 4 different experts.
All inputs are finite; a program needn't handle non-finite values.
Results may differ from the reference program's by a relative error of at most 0.005.
Values may be sent and summed in bfloat16 or wider, within the bound.
A program may use at most 128 MiB of HBM per device.

```python
import math
import jax
import jax.numpy as jnp
import numpy as np
from jax import lax

D = 2880
FF_WIN = 1440
TOP = 4
SHARD = 4
TOK_DEV = 64
EXPERTS = 16
FF_DEV = 360
CAP = 20
TOKENS = 4096
N_EP = 64


def level_of(own_key, extent, pieces, least, high):
    def one(axis_at, shards_of):
        steps = jax.random.uniform(jax.random.fold_in(jax.random.fold_in(own_key, 6), axis_at), (shards_of,), jnp.float32, least / len(pieces), high / len(pieces))
        return jnp.repeat(jnp.exp(steps), extent[axis_at] // shards_of).reshape((-1,) + (1,) * (len(extent) - axis_at - 1))

    level = one(*pieces[0])
    for cut in pieces[1:]:
        level = level * one(*cut)
    return level


def assign_block(own_key, own, number, rows, number_of, top, reach, slope):
    order = jax.random.permutation(own_key, number_of)
    heavy_load, usual = load_shares(number_of, rows * top, reach, slope, True), load_shares(number_of, rows * top, reach, slope, False)
    places = jnp.arange(number_of)

    def named(lengths, turn):
        used = int((lengths > 0).sum())
        fixed = max(1, used // 4)
        shifted = fixed + (places - fixed + turn * (used - fixed)) % max(1, number_of - fixed)
        return jnp.zeros((number_of,), jnp.int32).at[order[jnp.where(places < fixed, places, shifted)]].set(jnp.asarray(lengths, jnp.int32))

    lengths = jnp.where(number % 4 == 0, named(heavy_load, number // 4), named(usual, number - number // 4 - 1))
    mixed = jax.random.permutation(jax.random.fold_in(own, 3), number_of)
    source_of, receiver = mixed[0:number_of // 2 * 2:2], mixed[1:number_of // 2 * 2:2]
    margin = jnp.minimum(lengths[source_of] - 1, reach - lengths[receiver]) // 2
    margin = jnp.where((source_of == order[0]) | (receiver == order[0]) | (lengths[receiver] == 0), 0, jnp.maximum(margin, 0))
    shifted = jax.random.randint(jax.random.fold_in(own, 4), (number_of // 2,), 0, 1 << 20) % (margin + 1)
    lengths = lengths.at[source_of].add(-shifted).at[receiver].add(shifted)
    members = jnp.searchsorted(jnp.cumsum(lengths), jnp.arange(rows * top), side="right").astype(jnp.int32)
    table = members.reshape(top, rows).T
    table = table[jax.random.permutation(jax.random.fold_in(own, 1), rows)]
    turn = jax.random.randint(jax.random.fold_in(own, 2), (rows, 1), 0, top)
    return jnp.take_along_axis(table, (jnp.arange(top)[None, :] + turn) % top, axis=1)


def load_shares(number_of, total, reach, lean, full):
    portions = [(1 << 20) // math.isqrt(standing ** lean) + 1 for standing in range(1, number_of + 1)]
    largest = reach if full else min(reach, max(-(-total // number_of), total * portions[0] // sum(portions)))
    least = 1 if total - largest >= number_of - 1 else 0
    given, rest = [largest] + [least] * (number_of - 1), total - largest - least * (number_of - 1)
    while rest > 0:
        free = [i for i in range(1, number_of) if given[i] < largest] or [i for i in range(1, number_of) if given[i] < reach]
        whole, left = sum([portions[i] for i in free]), rest
        for i in free:
            more = min(reach - given[i], max(1, left * portions[i] // whole), rest)
            given[i] = given[i] + more
            rest = rest - more
    return np.array(given)


def centred(stream_key, shape, width, reach, cuts=(), held_as=jnp.bfloat16):
    values = width * jax.random.normal(stream_key, shape, jnp.float32)
    if cuts:
        values = values * level_of(stream_key, shape, cuts, -0.22, 0.18)
    return jnp.clip(values, -reach, reach).astype(held_as)


def setup_inputs(seed: int = 0, part: int = 0) -> dict:
    streams_of = jax.random.split(jax.random.key(seed), 7)
    own_keys = jax.random.split(jax.random.fold_in(streams_of[6], part), 7)
    tokens = centred(own_keys[0], (TOKENS, D), 1.0, 6.0, ((0, 64),))
    routes_keys = jax.random.split(jax.random.fold_in(own_keys[1], 1), TOKENS // TOK_DEV)
    routes_turns = jax.random.permutation(jax.random.fold_in(own_keys[1], 3), TOKENS // TOK_DEV)
    routes = jax.vmap(lambda own, number: assign_block(jax.random.fold_in(own_keys[1], 2), own, number, TOK_DEV, EXPERTS, TOP, CAP, 2))(routes_keys, routes_turns).reshape((TOKENS, TOP))
    norm_gain = jnp.clip(1.0 + 0.15 * jax.random.normal(streams_of[2], (D,), jnp.float32), 0.25, 1.75).astype(jnp.bfloat16)
    router_weight = centred(streams_of[3], (D, EXPERTS), (16 * D) ** -0.5, 0.02734375)
    gate_up_weight = centred(streams_of[4], (EXPERTS * SHARD, D, 2 * FF_DEV), D ** -0.5, 0.109375, ((0, 64),))
    down_weight = centred(streams_of[5], (EXPERTS * SHARD, FF_DEV, D), FF_WIN ** -0.5, 0.15625, ((0, 64),))
    return dict(tokens=tokens, routes=routes, norm_gain=norm_gain, router_weight=router_weight, gate_up_weight=gate_up_weight, down_weight=down_weight)


def reference(tokens, routes, norm_gain, router_weight, gate_up_weight, down_weight):
    stream = tokens.astype(jnp.float32)
    mean_square = lax.optimization_barrier(jnp.mean(stream * stream, axis=-1, keepdims=True))
    normed = (stream * lax.rsqrt(mean_square + 1e-05) * norm_gain.astype(jnp.float32)).astype(jnp.bfloat16)
    logits = jnp.dot(normed, router_weight, preferred_element_type=jnp.float32)
    expert_ids = jnp.arange(EXPERTS, dtype=jnp.int32)
    onehot = routes[:, :, None] == expert_ids[None, None, :]
    chosen = lax.optimization_barrier(jnp.sum(jnp.where(onehot, logits[:, None, :], jnp.float32(0.0)), axis=-1))
    expo = jnp.exp(chosen)
    route_prob = expo / lax.optimization_barrier(jnp.sum(expo, axis=-1, keepdims=True))
    flat_hits = onehot.astype(jnp.int32).reshape(N_EP, TOK_DEV * TOP, EXPERTS)
    rank_before = jnp.cumsum(flat_hits, axis=1) - flat_hits
    slot_index = lax.optimization_barrier(jnp.sum(flat_hits * rank_before, axis=-1)).reshape(TOKENS, TOP).astype(jnp.int32)
    block_ids = (jnp.arange(TOKENS, dtype=jnp.int32) // TOK_DEV)[:, None]
    position = (block_ids * CAP + slot_index).astype(jnp.int32)
    values = jnp.broadcast_to(normed[:, None, :], (TOKENS, TOP, D))
    buffer = jnp.zeros((EXPERTS, N_EP * CAP, D), jnp.bfloat16).at[routes, position].set(values)
    gate_up_all = gate_up_weight.reshape(EXPERTS, SHARD, D, 2 * FF_DEV)
    down_all = down_weight.reshape(EXPERTS, SHARD, FF_DEV, D)

    def one_expert(operands):
        rows, gate_up_part, down_part = operands
        total = jnp.zeros((N_EP * CAP, D), jnp.float32)
        for member in range(SHARD):
            hidden = jnp.dot(rows, gate_up_part[member], preferred_element_type=jnp.float32)
            gate_part = hidden[:, :FF_DEV]
            up_part = hidden[:, FF_DEV:]
            activated = ((up_part + 1.0) * gate_part * jax.nn.sigmoid(1.702 * gate_part)).astype(jnp.bfloat16)
            partial_value = jnp.dot(activated, down_part[member], preferred_element_type=jnp.float32).astype(jnp.bfloat16)
            total = total + partial_value.astype(jnp.float32)
        return total
    expert_sum = lax.map(one_expert, (buffer, gate_up_all, down_all))
    mixture = jnp.zeros((TOKENS, D), jnp.float32)
    for choice_k in range(TOP):
        picked = expert_sum[routes[:, choice_k], position[:, choice_k]]
        mixture = mixture + route_prob[:, choice_k:choice_k + 1] * picked
    return (stream + mixture).astype(jnp.bfloat16)
```

```python
import jax
import jax.numpy as jnp
from jax import lax
from jax.sharding import Mesh
from jax.sharding import PartitionSpec as P

EP = ("ep_0", "ep_1")
GROUPS_EP = ("groups", "ep_0", "ep_1")


def shards(tokens, routes, norm_gain, router_weight, gate_up_weight, down_weight):
    experts = router_weight.shape[1]
    devices = lax.axis_size(EP)
    shard_count = devices // experts
    ff_dev = down_weight.shape[1]
    stream = tokens.astype(jnp.float32)
    mean_square = jnp.mean(stream * stream, axis=-1, keepdims=True)
    normed = (stream * lax.rsqrt(mean_square + 1e-05) * norm_gain.astype(jnp.float32)).astype(
        jnp.bfloat16
    )
    rows_in = lax.all_gather(normed, EP, axis=0, tiled=True)
    logits = jnp.dot(normed, router_weight, preferred_element_type=jnp.float32)
    expert_ids = lax.broadcasted_iota(jnp.int32, (1, 1, experts), 2)
    onehot = routes[:, :, None] == expert_ids
    chosen = jnp.sum(jnp.where(onehot, logits[:, None, :], jnp.float32(0.0)), axis=-1)
    expo = jnp.exp(chosen)
    route_prob = expo / jnp.sum(expo, axis=-1, keepdims=True)
    weight = jnp.sum(jnp.where(onehot, route_prob[:, :, None], jnp.float32(0.0)), axis=1)
    weights = lax.all_gather(weight.T, EP, axis=1, tiled=True)
    my_expert = lax.axis_index(EP) // shard_count
    mine = lax.dynamic_slice_in_dim(weights, my_expert, 1, axis=0).reshape(-1, 1)
    hidden = jnp.dot(rows_in, gate_up_weight[0], preferred_element_type=jnp.float32)
    gate_part = hidden[:, :ff_dev]
    up_part = hidden[:, ff_dev:]
    activated = ((up_part + 1.0) * gate_part * jax.nn.sigmoid(1.702 * gate_part)).astype(
        jnp.bfloat16
    )
    partial_value = jnp.dot(activated, down_weight[0], preferred_element_type=jnp.float32)
    share = jnp.where(mine != 0.0, partial_value * mine, jnp.float32(0.0)).astype(jnp.bfloat16)
    mixture = lax.psum_scatter(share, EP, scatter_dimension=0, tiled=True)
    return (stream + mixture.astype(jnp.float32)).astype(jnp.bfloat16)


def solution(mesh):
    split = Mesh(mesh.devices.reshape(mesh.shape["groups"], 32, 2), ("groups", "ep_0", "ep_1"))
    placed = (
        P(GROUPS_EP, None),
        P(GROUPS_EP, None),
        P(),
        P(),
        P(EP, None, None),
        P(EP, None, None),
    )
    return jax.shard_map(
        shards, mesh=split, in_specs=placed, out_specs=P(GROUPS_EP, None), check_vma=False
    )
```

```python
import functools

import jax
import jax.numpy as jnp
from jax import lax
from jax.experimental import pallas as pl
from jax.experimental.pallas import tpu as pltpu
from jax.sharding import PartitionSpec as P

MESH = pl.DeviceIdType.MESH
CORES = 2
CHUNK = 16
DIRS = 2
F32, BF16 = jnp.float32, jnp.bfloat16


def reach_limits(tok_rows, top_count, experts, shard_count):
    capacity = min(
        tok_rows, shard_count * (17 * tok_rows * top_count // (16 * experts * shard_count) + 1)
    )
    half = experts // 2

    def chunks_at(hop):
        offset = (hop + 1) // 2
        return pl.cdiv(min(tok_rows, (half - offset + 1) * capacity), CHUNK)

    hops = range(1, 2 * half)
    return [max(h for h in hops if chunks_at(h) > q) for q in range(tok_rows // CHUNK)]


def kernel(
    limits,
    experts,
    shard_count,
    tokens_ref,
    routes_ref,
    gain_ref,
    router_ref,
    gate_up_ref,
    down_ref,
    out_ref,
    rows_buf,
    share_buf,
    back_buf,
    gate_up_buf,
    down_buf,
    act_buf,
    place_buf,
    local_sem,
    pair_send,
    pair_recv,
    go_send,
    go_recv,
    back_send,
    back_recv,
):
    chips = lax.axis_size("ep") // CORES
    last = chips // 2
    tok_rows, width = tokens_ref.shape
    top_count = routes_ref.shape[1]
    wide = rows_buf.shape[2]
    ff_dev = down_ref.shape[1]
    aligned = wide - 128
    me = lax.axis_index("ep")
    chip, core = me // CORES, me % CORES
    my_expert = me // shard_count
    sibling = chip * CORES + (1 - core)
    ahead = lax.rem(chip + 1, chips) * CORES + core
    behind = lax.rem(chip + chips - 1, chips) * CORES + core

    def to(device):
        return {"ep": device}

    own_copies = [
        pltpu.make_async_copy(gate_up_ref.at[0], gate_up_buf.at[0, pl.ds(0, width)], local_sem.at[0]),
        pltpu.make_async_copy(down_ref.at[0], down_buf.at[0], local_sem.at[1]),
    ]
    for copy in own_copies:
        copy.start()
    barrier = pltpu.get_barrier_semaphore()
    for device in (sibling, ahead, behind):
        pl.semaphore_signal(barrier, inc=1, device_id=to(device), device_id_type=MESH)

    stream = tokens_ref[...].astype(F32)
    mean_square = jnp.sum(stream * stream, axis=1, keepdims=True) / width
    normed = (stream * lax.rsqrt(mean_square + 1e-05) * gain_ref[...].astype(F32)).astype(BF16)
    logits = jnp.dot(normed, router_ref[...], preferred_element_type=F32)
    routes = routes_ref[...]
    expert_ids = lax.broadcasted_iota(jnp.int32, (tok_rows, experts), 1)
    picks = [routes[:, k : k + 1] == expert_ids for k in range(top_count)]
    expo = [
        jnp.exp(jnp.sum(jnp.where(pick, logits, 0.0), axis=1, keepdims=True)) for pick in picks
    ]
    total = expo[0]
    for value in expo[1:]:
        total = total + value
    weight = jnp.zeros((tok_rows, experts), F32)
    for pick, value in zip(picks, expo):
        weight = weight + jnp.where(pick, value / total, 0.0)

    high = weight.astype(BF16)
    rest = weight - high.astype(F32)
    middle = rest.astype(BF16)
    low = (rest - middle.astype(F32)).astype(BF16)
    tail_width = width - aligned

    def shift_to(start, count):
        source = lax.broadcasted_iota(jnp.int32, (count, 128), 0)
        target = lax.broadcasted_iota(jnp.int32, (count, 128), 1)
        return jnp.where(target == source + start, 1.0, 0.0).astype(BF16)

    tail = jnp.dot(normed[:, aligned:], shift_to(0, tail_width), preferred_element_type=F32)
    for place, piece in enumerate((high, middle, low)):
        tail = tail + jnp.dot(
            piece, shift_to(tail_width + place * experts, experts), preferred_element_type=F32
        )
    tail = tail.astype(BF16)

    row_id = lax.broadcasted_iota(jnp.int32, (tok_rows, tok_rows), 0)
    col_id = lax.broadcasted_iota(jnp.int32, (tok_rows, tok_rows), 1)
    half = experts // 2
    for way in range(DIRS):
        distance = routes - my_expert if way == 0 else my_expert - routes
        distance = jnp.where(distance < 0, distance + experts, distance)
        distance = jnp.where(distance <= half, distance, 0).astype(F32)
        key = jnp.max(distance, axis=1, keepdims=True)
        key_row = jnp.sum(jnp.where(row_id == col_id, key, 0.0), axis=0, keepdims=True)
        first = (key_row > key) | ((key_row == key) & (col_id < row_id))
        rank = jnp.sum(jnp.where(first, 1.0, 0.0), axis=1, keepdims=True)
        place_buf[way] = jnp.where(rank == col_id.astype(F32), 1.0, 0.0).astype(BF16)
        later = (key > key_row) | ((key == key_row) & (row_id < col_id))
        rank_row = jnp.sum(jnp.where(later, 1.0, 0.0), axis=0, keepdims=True)
        order = jnp.where(rank_row == row_id.astype(F32), 1.0, 0.0).astype(BF16)
        rows = pl.ds(way * tok_rows, tok_rows)
        rows_buf[0, rows, :aligned] = jnp.dot(
            order, normed[:, :aligned], preferred_element_type=F32
        ).astype(BF16)
        rows_buf[0, rows, aligned:] = jnp.dot(order, tail, preferred_element_type=F32).astype(BF16)
    spare = 1 - lax.rem(chip, 2)
    spare_rows = pl.ds(pl.multiple_of(spare * tok_rows, tok_rows), tok_rows)
    rows_buf[last, spare_rows, :] = rows_buf[0, spare_rows, :]
    for shard in range(CORES):
        gate_up_buf[shard, width:, :] = jnp.zeros(
            (gate_up_buf.shape[1] - width, gate_up_buf.shape[2]), BF16
        )

    def chunk_rows(way, q):
        return pl.ds(way * tok_rows + q * CHUNK, CHUNK)

    def go(way, hop, q):
        return pltpu.make_async_remote_copy(
            src_ref=rows_buf.at[hop - 1, chunk_rows(way, q)],
            dst_ref=rows_buf.at[hop, chunk_rows(way, q)],
            send_sem=go_send.at[way, hop - 1, q],
            recv_sem=go_recv.at[way, hop - 1, q],
            device_id=to(ahead if way == 0 else behind),
            device_id_type=MESH,
        )

    def back(way, hop, q):
        return pltpu.make_async_remote_copy(
            src_ref=share_buf.at[hop, chunk_rows(way, q)],
            dst_ref=back_buf.at[hop - 1, chunk_rows(way, q)],
            send_sem=back_send.at[way, hop - 1, q],
            recv_sem=back_recv.at[way, hop - 1, q],
            device_id=to(behind if way == 0 else ahead),
            device_id_type=MESH,
        )

    def limit(way, hop, q):
        odd = lax.rem(chip + hop, 2)
        return limits[q] + (1 - odd if way == 0 else odd)

    chunks = [(q, way) for q in range(len(limits)) for way in range(DIRS)]

    pl.semaphore_wait(barrier, 3)
    for q, way in chunks:
        go(way, 1, q).start()
    pair_copies = [
        pltpu.make_async_remote_copy(
            src_ref=source,
            dst_ref=target,
            send_sem=pair_send.at[at],
            recv_sem=pair_recv.at[at],
            device_id=to(sibling),
            device_id_type=MESH,
        )
        for at, (source, target) in enumerate(
            (
                (gate_up_ref.at[0], gate_up_buf.at[1, pl.ds(0, width)]),
                (down_ref.at[0], down_buf.at[1]),
            )
        )
    ]
    for copy in pair_copies:
        copy.start()

    def up_piece(slot, shard):
        hidden = jnp.dot(rows_buf[slot], gate_up_buf[shard], preferred_element_type=F32)
        gate = hidden[:, :ff_dev]
        up = hidden[:, ff_dev:]
        act_buf[shard] = ((up + 1.0) * gate * jax.nn.sigmoid(1.702 * gate)).astype(BF16)

    def down_piece(slot, start, stop):
        lane = lax.broadcasted_iota(jnp.int32, (DIRS * tok_rows, 128), 1)
        mine = (
            (lane == tail_width + my_expert)
            | (lane == tail_width + experts + my_expert)
            | (lane == tail_width + 2 * experts + my_expert)
        )
        parts = rows_buf[slot, :, aligned:].astype(F32)
        factor = jnp.sum(jnp.where(mine, parts, 0.0), axis=1, keepdims=True)
        value = jnp.dot(act_buf[0], down_buf[0, :, start:stop], preferred_element_type=F32)
        value = value + jnp.dot(act_buf[1], down_buf[1, :, start:stop], preferred_element_type=F32)
        share_buf[slot, :, start:stop] = jnp.where(factor != 0.0, value * factor, 0.0).astype(BF16)

    middle_column = 256 * (width // 512 + 1)

    def piece(slot, part):
        if part < CORES:
            up_piece(slot, part)
        elif part == CORES:
            down_piece(slot, 0, middle_column)
        else:
            down_piece(slot, middle_column, width)

    def gather_step(hop, carry):
        for q in range(len(limits)):
            for way in range(DIRS):
                bound = limit(way, hop, q)

                @pl.when(hop <= bound)
                def _():
                    go(way, hop, q).wait_recv()

                @pl.when(hop + 1 <= bound)
                def _():
                    go(way, hop + 1, q).start()

            if q < len(limits) - 1:

                @pl.when(hop >= 2)
                def _():
                    piece(hop - 1, q + 1)
            else:

                @pl.when(hop == 1)
                def _():
                    for copy in own_copies:
                        copy.wait()
                    for copy in pair_copies:
                        copy.wait_recv()

                @pl.when(hop <= last)
                def _():
                    piece(hop, 0)

        return carry

    lax.fori_loop(1, last + 2, gather_step, 0)

    def return_step(step, carry):
        hop = last - step
        for q in range(len(limits)):
            for way in range(DIRS):
                bound = limit(way, hop, q)
                rows = chunk_rows(way, q)

                @pl.when(hop + 1 <= bound)
                def _():
                    back(way, hop + 1, q).wait_recv()
                    share_buf[hop, rows, :] = (
                        share_buf[hop, rows, :].astype(F32) + back_buf[hop, rows, :].astype(F32)
                    ).astype(BF16)

            for way in range(DIRS):
                bound = limit(way, hop, q)

                @pl.when(hop <= bound)
                def _():
                    back(way, hop, q).start()

        return carry

    lax.fori_loop(0, last, return_step, 0)

    def drain_step(hop, carry):
        for q, way in chunks:
            @pl.when(hop + 1 <= limit(way, hop, q))
            def _():
                go(way, hop + 1, q).wait_send()

            @pl.when((hop >= 1) & (hop <= limit(way, hop, q)))
            def _():
                back(way, hop, q).wait_send()

        return carry

    for q, way in chunks:
        back(way, 1, q).wait_recv()
    own = jnp.where(spare == 0, place_buf[0].astype(F32), place_buf[1].astype(F32)).astype(BF16)
    mixture = jnp.dot(own, share_buf[last, spare_rows, :], preferred_element_type=F32)
    for way in range(DIRS):
        mixture = mixture + jnp.dot(
            place_buf[way],
            back_buf[0, pl.ds(way * tok_rows, tok_rows), :],
            preferred_element_type=F32,
        )
    out_ref[...] = (tokens_ref[...].astype(F32) + mixture).astype(out_ref.dtype)
    lax.fori_loop(0, last + 1, drain_step, 0)
    for copy in pair_copies:
        copy.wait_send()


def shards(tokens, routes, norm_gain, router_weight, gate_up_weight, down_weight):
    tok_rows, width = tokens.shape
    experts = router_weight.shape[1]
    devices = lax.axis_size("ep")
    shard_count = devices // experts
    chips = devices // CORES
    ff_dev = down_weight.shape[1]
    limits = reach_limits(tok_rows, routes.shape[1], experts, shard_count)
    wide = width + 64
    last = chips // 2
    vmem = pl.BlockSpec(memory_space=pltpu.VMEM)
    hbm = pl.BlockSpec(memory_space=pl.ANY)
    copies = pltpu.SemaphoreType.DMA((DIRS, last, len(limits)))
    return pl.pallas_call(
        functools.partial(kernel, limits, experts, shard_count),
        out_shape=jax.ShapeDtypeStruct((tok_rows, width), BF16),
        in_specs=[vmem, vmem, vmem, vmem, hbm, hbm],
        out_specs=vmem,
        scratch_shapes=[
            pltpu.VMEM((last + 1, DIRS * tok_rows, wide), BF16),
            pltpu.VMEM((last + 1, DIRS * tok_rows, width), BF16),
            pltpu.VMEM((last, DIRS * tok_rows, width), BF16),
            pltpu.VMEM((CORES, wide, 2 * ff_dev), BF16),
            pltpu.VMEM((CORES, ff_dev, width), BF16),
            pltpu.VMEM((CORES, DIRS * tok_rows, ff_dev), BF16),
            pltpu.VMEM((DIRS, tok_rows, tok_rows), BF16),
            pltpu.SemaphoreType.DMA((2,)),
            pltpu.SemaphoreType.DMA((2,)),
            pltpu.SemaphoreType.DMA((2,)),
            copies,
            copies,
            copies,
            copies,
        ],
        compiler_params=pltpu.CompilerParams(
            collective_id=0, has_side_effects=True, vmem_limit_bytes=60 * 1024 * 1024
        ),
    )(tokens, routes, norm_gain.reshape(1, width), router_weight, gate_up_weight, down_weight)


def solution(mesh):
    rows = P(("groups", "ep"), None)
    return jax.shard_map(
        shards,
        mesh=mesh,
        in_specs=(rows, rows, P(), P(), P("ep", None, None), P("ep", None, None)),
        out_specs=rows,
        check_vma=False,
    )
```
